256 devices in a mesh: seq: 16 (over z, core), feat: 16 (over y, x).
Axes of the slice: x: 4, y: 4, z: 8, core: 2. Of those that a mesh axis runs over, the one named last changes fastest.
Arguments:
- layer_inputs: bfloat16 [128, 256, 8192], P('seq', None, 'feat'), may hold values from -6 to 6
- out_grads: bfloat16 [128, 256, 28672], P('seq', None, 'feat'), may hold values from -6 to 6
- lengths: int32 [128], P('seq'), may hold values from 1 to 256, 20480 in all
- row_order: int32 [128], P('seq'), may hold values from 0 to 127, each once
- query_in: bfloat16 [8192, 512], P('feat'), may hold values from -0.005859375 to 0.005859375
- query_out: bfloat16 [28672, 512], P('feat'), may hold values from -0.0029296875 to 0.0029296875
Outputs:
- scores: float32 [128, 16], P('seq')
The draws below stay inside these ranges and needn't reach their ends.
Inputs may be any that keep to these rules, and one draw needn't show every extreme that they name: `lengths`: slots at or past a sequence's length hold padding. `row_order`: each sequence number appears exactly once.
All inputs are finite; a program needn't handle non-finite values. No bound on the sum of `lengths` on one device may be relied on, other than what follows from the above.
Results may differ from the reference program's by a relative error of at most 0.018.
Values may be sent and summed in bfloat16 or wider, within the bound.
A program may use at most 64 MiB of HBM per device.

```python
import math
import jax
import jax.numpy as jnp
import numpy as np
from jax import lax

D = 8192
FF = 28672
Q = 16
R = 32
LEN = 256
SEQ_DEV = 8
SEQS = 128
FEAT_GROUPS = 16
N_SEQ = 16


def block_scale(rng, extent, split, low, top_value):
    factor_of, own = 1.0, jax.random.fold_in(rng, 6)
    for dim, shards_of in split:
        draws = jnp.exp(jax.random.uniform(jax.random.fold_in(own, dim), (shards_of,), jnp.float32, low / len(split), top_value / len(split)))
        factor_of = factor_of * jnp.repeat(draws, extent[dim] // shards_of).reshape([-1 if axis == dim else 1 for axis in range(len(extent))])
    return factor_of


def profile(count, total, limit, lean):
    loads = [(1 << 20) // math.isqrt(standing ** lean) + 1 for standing in range(2, count + 1)]
    spare, holding = total - limit - (count - 1), [1] * (count - 1)
    while spare > 0:
        free = [i for i in range(count - 1) if holding[i] < limit]
        mass, budget = sum([loads[i] for i in free]), spare
        for i in free:
            addition = min(limit - holding[i], max(1, budget * loads[i] // mass), spare)
            holding[i] = holding[i] + addition
            spare = spare - addition
    return np.array([limit] + holding)


def uneven_parts(stream_key, count, total, limit, lean):
    if count == 2:
        one = jax.random.randint(stream_key, (), max(1, total - limit), min(limit, total - 1) + 1)
        return jnp.stack([one, total - one])
    tallies = jnp.asarray(profile(count, total, limit, lean), jnp.int32)
    twos = (count - 1) // 2
    giver, sink = tallies[1:1 + 2 * twos:2], tallies[2:2 + 2 * twos:2]
    slack = jnp.minimum(giver - 1, limit - sink)
    passed = jax.random.randint(jax.random.fold_in(stream_key, 1), (twos,), 0, 1 << 20) % (slack + 1)
    tallies = tallies.at[1:1 + 2 * twos:2].set(giver - passed).at[2:2 + 2 * twos:2].set(sink + passed)
    return tallies[jax.random.permutation(jax.random.fold_in(stream_key, 2), count)]


def bell_draw(key, shape, spread, most, shards=(), kind=jnp.bfloat16):
    level = block_scale(key, shape, shards, -0.22, 0.18) if shards else 1.0
    array = jax.random.normal(key, shape, jnp.float32) * spread * level
    return jnp.minimum(jnp.maximum(array, -most), most).astype(kind)


def setup_inputs(seed: int = 0) -> dict:
    arg_keys = jax.random.split(jax.random.key(seed), 7)
    layer_inputs = bell_draw(arg_keys[0], (SEQS, LEN, D), 1.0, 6.0, ((0, 16), (2, 16)))
    out_grads = bell_draw(arg_keys[1], (SEQS, LEN, FF), 1.0, 6.0, ((0, 16), (2, 16)))
    lengths = uneven_parts(arg_keys[2], SEQS, SEQ_DEV * N_SEQ * LEN * 5 // 8, LEN, 2).astype(jnp.int32)
    row_order = jax.random.permutation(arg_keys[3], SEQS).astype(jnp.int32)
    query_in = bell_draw(arg_keys[4], (D, Q * R), (D * 128) ** -0.5, 0.005859375, ((0, 16),))
    query_out = bell_draw(arg_keys[5], (FF, Q * R), (FF * 128) ** -0.5, 0.0029296875, ((0, 16),))
    return dict(layer_inputs=layer_inputs, out_grads=out_grads, lengths=lengths, row_order=row_order, query_in=query_in, query_out=query_out)


def reference(layer_inputs, out_grads, lengths, row_order, query_in, query_out):
    row_total = SEQS * LEN
    columns = Q * R
    width_in = D // FEAT_GROUPS
    width_out = FF // FEAT_GROUPS
    flat_in = layer_inputs.reshape(row_total, D)
    flat_out = out_grads.reshape(row_total, FF)

    def add_block(shard_index, running):
        shard_index = jnp.asarray(shard_index).astype(jnp.int32)
        part_in = lax.dynamic_slice_in_dim(flat_in, shard_index * width_in, width_in, 1)
        part_out = lax.dynamic_slice_in_dim(flat_out, shard_index * width_out, width_out, 1)
        factor_in = lax.dynamic_slice_in_dim(query_in, shard_index * width_in, width_in, 0)
        factor_out = lax.dynamic_slice_in_dim(query_out, shard_index * width_out, width_out, 0)
        block_terms = jnp.concatenate(
            [jnp.dot(part_in, factor_in, preferred_element_type=jnp.float32),
             jnp.dot(part_out, factor_out, preferred_element_type=jnp.float32)], axis=1).astype(jnp.bfloat16)
        block_terms = lax.optimization_barrier(block_terms)
        return running + block_terms.astype(jnp.float32)

    projected = lax.fori_loop(0, FEAT_GROUPS, add_block, jnp.zeros((row_total, 2 * columns), jnp.float32))
    products = (projected[:, :columns] * projected[:, columns:]).reshape(SEQS, LEN, columns)
    is_live = (jnp.arange(LEN, dtype=jnp.int32)[None, :] < lengths[:, None]).astype(jnp.float32)
    seq_sums = jnp.sum(products * is_live[:, :, None], axis=1)
    seq_scores = seq_sums.reshape(SEQS, Q, R).sum(axis=2)
    return jnp.take(seq_scores, row_order, axis=0)
```

```python
import functools

import jax
import jax.numpy as jnp
from jax import lax
from jax.experimental import pallas as pl
from jax.experimental.pallas import tpu as pltpu
from jax.sharding import PartitionSpec as P

Q = 16
R = 32
SIDE = 4
LANES = 128
OFFS = (2, 1, 3, 0)
BF16 = jnp.bfloat16
F32 = jnp.float32


def kernel(n_seq, lengths, row_order, li, og, qi, qo, out,
           xb, gb, wi, wo, part, rec1, acc1, mid, rec2, acc2, tile, gz, mine, gp,
           load_sem, s1_send, s1_recv, s2_send, s2_recv, gz_sem, gp_sem):
    n_feat = SIDE * SIDE
    me_s = lax.axis_index("seq")
    me_f = lax.axis_index("feat")
    y = me_f // SIDE
    x = me_f % SIDE
    rows = xb.shape[2]
    seq_dev = li.shape[0]

    def neighbour(axis, step):
        if axis == 0:
            return y * SIDE + lax.rem(x + step, SIDE)
        return lax.rem(y + step, SIDE) * SIDE + x

    pos = (x, y)

    barrier = pltpu.get_barrier_semaphore()
    for d in range(1, n_feat):
        pl.semaphore_signal(barrier, inc=1, device_id={"feat": lax.rem(me_f + d, n_feat)},
                            device_id_type=pl.DeviceIdType.MESH)
    for d in range(1, n_seq):
        pl.semaphore_signal(barrier, inc=1, device_id={"seq": lax.rem(me_s + d, n_seq)},
                            device_id_type=pl.DeviceIdType.MESH)

    def seq_of(h, t):
        return h * SIDE + lax.rem(pos[1 - h] + OFFS[t], SIDE)

    def load_x(h, t):
        return pltpu.make_async_copy(li.at[seq_of(h, t)], xb.at[h, t], load_sem.at[2 + h * 8 + t * 2])

    def load_g(h, t):
        return pltpu.make_async_copy(og.at[seq_of(h, t)], gb.at[h, t], load_sem.at[3 + h * 8 + t * 2])

    load_wi = pltpu.make_async_copy(qi, wi, load_sem.at[0])
    load_wo = pltpu.make_async_copy(qo, wo, load_sem.at[1])
    load_wi.start()
    load_x(0, 0).start()
    load_x(1, 0).start()
    load_wo.start()
    load_g(0, 0).start()
    load_g(1, 0).start()
    for h in range(2):
        load_x(h, 1).start()
        load_g(h, 1).start()

    def send(src, dst, ssem, rsem, target):
        copy = pltpu.make_async_remote_copy(
            src_ref=src, dst_ref=dst, send_sem=ssem, recv_sem=rsem,
            device_id={"feat": target}, device_id_type=pl.DeviceIdType.MESH)
        return copy

    def ring_copy(axis, slot, src, rec, ssem, rsem):
        step = 1 if slot in (0, 2, 5) else SIDE - 1
        return send(src, rec.at[slot], ssem.at[slot], rsem.at[slot], neighbour(axis, step))

    def tile_in(h, t, step):
        return part.at[h, t, lax.rem(pos[h] + step, SIDE)]

    def tile_out(h, t, step):
        return part.at[h, t, SIDE + lax.rem(pos[h] + step, SIDE)]

    def copy1(h, t, slot):
        if slot >= 4:
            src = acc1.at[h, t, slot - 4]
        elif slot in (0, 3):
            src = tile_in(h, t, 1 if slot == 0 else 2)
        else:
            src = tile_out(h, t, 3 if slot == 1 else 2)
        return ring_copy(h, slot, src, rec1.at[h, t], s1_send.at[h, t], s1_recv.at[h, t])

    def copy2(h, slot):
        src = (mid.at[h, 1, 0], mid.at[h, 2, 1], mid.at[h, 0, 1], mid.at[h, 0, 0], acc2.at[h, 0], acc2.at[h, 1])[slot]
        return ring_copy(1 - h, slot, src, rec2.at[h], s2_send.at[h], s2_recv.at[h])

    def added(*refs):
        total = refs[0][...].astype(F32)
        for ref in refs[1:]:
            total = total + ref[...].astype(F32)
        return total

    def compute_in(h, t):
        load_x(h, t).wait()
        value = jnp.dot(xb[h, t], wi[...], preferred_element_type=F32).astype(BF16)
        for c in range(SIDE):
            part[h, t, c] = value[:, c * LANES:(c + 1) * LANES]

    def compute_out(h, t):
        load_g(h, t).wait()
        value = jnp.dot(gb[h, t], wo[...], preferred_element_type=F32).astype(BF16)
        for c in range(SIDE):
            part[h, t, SIDE + c] = value[:, c * LANES:(c + 1) * LANES]

    def accumulate1(h, t):
        copy1(h, t, 3).wait_recv()
        acc1[h, t, 0] = added(tile_in(h, t, 3), rec1.at[h, t, 3]).astype(BF16)
        copy1(h, t, 4).start()
        copy1(h, t, 2).wait_recv()
        acc1[h, t, 1] = added(tile_out(h, t, 1), rec1.at[h, t, 2]).astype(BF16)
        copy1(h, t, 5).start()

    def final1(h, t):
        copy1(h, t, 0).wait_recv()
        copy1(h, t, 4).wait_recv()
        mid[h, t, 0] = added(tile_in(h, t, 0), rec1.at[h, t, 0], rec1.at[h, t, 4]).astype(BF16)
        copy1(h, t, 1).wait_recv()
        copy1(h, t, 5).wait_recv()
        mid[h, t, 1] = added(tile_out(h, t, 0), rec1.at[h, t, 1], rec1.at[h, t, 5]).astype(BF16)

    def step(t):
        for h in range(2):
            compute_in(h, t)
            if t == 0 and h == 0:
                pl.semaphore_wait(barrier, n_feat - 1 + n_seq - 1)
            copy1(h, t, 3).start()
            copy1(h, t, 0).start()
        if t == 0:
            load_wo.wait()
        for h in range(2):
            compute_out(h, t)
            copy1(h, t, 2).start()
            copy1(h, t, 1).start()
        if t + 2 < SIDE:
            for h in range(2):
                load_x(h, t + 2).start()
                load_g(h, t + 2).start()

    load_wi.wait()
    step(0)
    step(1)
    for h in range(2):
        accumulate1(h, 0)
    step(2)
    for h in range(2):
        accumulate1(h, 1)
    for h in range(2):
        final1(h, 0)
        copy2(h, 3).start()
        copy2(h, 2).start()
    step(3)
    for h in range(2):
        accumulate1(h, 2)
    for h in range(2):
        final1(h, 1)
        copy2(h, 0).start()
    for h in range(2):
        accumulate1(h, 3)
    for h in range(2):
        copy2(h, 2).wait_recv()
        acc2[h, 1] = added(mid.at[h, 1, 1], rec2.at[h, 2]).astype(BF16)
        copy2(h, 5).start()
    for h in range(2):
        final1(h, 2)
        copy2(h, 1).start()
        copy2(h, 3).wait_recv()
        acc2[h, 0] = added(mid.at[h, 2, 0], rec2.at[h, 3]).astype(BF16)
        copy2(h, 4).start()

    row = lax.broadcasted_iota(jnp.int32, (seq_dev, rows), 1)
    seq_id = lax.broadcasted_iota(jnp.int32, (seq_dev, rows), 0)
    lane_from = lax.broadcasted_iota(jnp.int32, (LANES, LANES), 0)
    lane_to = lax.broadcasted_iota(jnp.int32, (LANES, LANES), 1)
    total = None
    for h in range(2):
        copy1(h, 3, 0).wait_recv()
        copy1(h, 3, 4).wait_recv()
        copy2(h, 0).wait_recv()
        copy2(h, 4).wait_recv()
        both_in = added(tile_in(h, 3, 0), rec1.at[h, 3, 0], rec1.at[h, 3, 4], rec2.at[h, 0], rec2.at[h, 4])
        copy1(h, 3, 1).wait_recv()
        copy1(h, 3, 5).wait_recv()
        copy2(h, 1).wait_recv()
        copy2(h, 5).wait_recv()
        both_out = added(tile_out(h, 3, 0), rec1.at[h, 3, 1], rec1.at[h, 3, 5], rec2.at[h, 1], rec2.at[h, 5])
        products = both_in * both_out
        which = seq_of(h, 3)
        live = (seq_id == which) & (row < lengths[which])
        sums = jnp.dot(live.astype(F32), products, precision=lax.Precision.HIGHEST, preferred_element_type=F32)
        place = (lane_to == pos[h] * (LANES // R) + lane_from // R).astype(F32)
        scored = jnp.dot(sums, place, precision=lax.Precision.HIGHEST, preferred_element_type=F32)
        total = scored if total is None else total + scored
    tile[...] = total
    gz[me_s] = total

    def spread_z(d):
        return pltpu.make_async_remote_copy(
            src_ref=tile, dst_ref=gz.at[me_s], send_sem=gz_sem.at[0], recv_sem=gz_sem.at[1],
            device_id={"seq": lax.rem(me_s + d, n_seq)}, device_id_type=pl.DeviceIdType.MESH)

    def spread_plane(d):
        return pltpu.make_async_remote_copy(
            src_ref=mine, dst_ref=gp.at[me_f], send_sem=gp_sem.at[0], recv_sem=gp_sem.at[1],
            device_id={"feat": lax.rem(me_f + d, n_feat)}, device_id_type=pl.DeviceIdType.MESH)

    def all_of(ref, sem, n, axis):
        return pltpu.make_async_remote_copy(
            src_ref=ref.at[pl.ds(0, n)], dst_ref=ref.at[pl.ds(0, n)], send_sem=sem.at[0], recv_sem=sem.at[1],
            device_id={axis: lax.axis_index(axis)}, device_id_type=pl.DeviceIdType.MESH)

    for d in range(1, n_seq):
        spread_z(d).start()
    wanted = jnp.zeros((seq_dev, seq_dev * n_seq), jnp.int32)
    out_row = lax.broadcasted_iota(jnp.int32, wanted.shape, 0)
    for i in range(seq_dev):
        wanted = jnp.where(out_row == i, row_order[i], wanted)
    picked = (wanted == lax.broadcasted_iota(jnp.int32, wanted.shape, 1)).astype(F32)
    if n_seq > 1:
        all_of(gz, gz_sem, n_seq - 1, "seq").wait_recv()
    every = gz[...].reshape(n_seq * seq_dev, LANES)
    own = jnp.dot(picked, every, precision=lax.Precision.HIGHEST, preferred_element_type=F32)
    mine[...] = own
    gp[me_f] = own
    for d in range(1, n_feat):
        spread_plane(d).start()
    for h in range(2):
        for t in range(SIDE):
            for slot in range(6):
                copy1(h, t, slot).wait_send()
        for slot in range(6):
            copy2(h, slot).wait_send()
    if n_seq > 1:
        all_of(gz, gz_sem, n_seq - 1, "seq").wait_send()
    all_of(gp, gp_sem, n_feat - 1, "feat").wait_recv()
    summed = gp[0]
    for f in range(1, n_feat):
        summed = summed + gp[f]
    out[...] = summed[:, :Q]
    all_of(gp, gp_sem, n_feat - 1, "feat").wait_send()


def on_device(n_seq, layer_inputs, out_grads, lengths, row_order, query_in, query_out):
    seq_dev, rows, width_in = layer_inputs.shape
    width_out = out_grads.shape[2]
    columns = query_in.shape[1]
    n_feat = SIDE * SIDE
    smem = pl.BlockSpec(memory_space=pltpu.SMEM)
    hbm = pl.BlockSpec(memory_space=pl.ANY)
    tile_of = (rows, LANES)
    return pl.pallas_call(
        functools.partial(kernel, n_seq),
        out_shape=jax.ShapeDtypeStruct((seq_dev, Q), F32),
        in_specs=[smem, smem, hbm, hbm, hbm, hbm],
        out_specs=pl.BlockSpec(memory_space=pltpu.VMEM),
        scratch_shapes=[
            pltpu.VMEM((2, SIDE, rows, width_in), BF16),
            pltpu.VMEM((2, SIDE, rows, width_out), BF16),
            pltpu.VMEM((width_in, columns), BF16),
            pltpu.VMEM((width_out, columns), BF16),
            pltpu.VMEM((2, SIDE, 2 * SIDE, *tile_of), BF16),
            pltpu.VMEM((2, SIDE, 6, *tile_of), BF16),
            pltpu.VMEM((2, SIDE, 2, *tile_of), BF16),
            pltpu.VMEM((2, SIDE, 2, *tile_of), BF16),
            pltpu.VMEM((2, 6, *tile_of), BF16),
            pltpu.VMEM((2, 2, *tile_of), BF16),
            pltpu.VMEM((seq_dev, LANES), F32),
            pltpu.VMEM((n_seq, seq_dev, LANES), F32),
            pltpu.VMEM((seq_dev, LANES), F32),
            pltpu.VMEM((n_feat, seq_dev, LANES), F32),
            pltpu.SemaphoreType.DMA((18,)),
            pltpu.SemaphoreType.DMA((2, SIDE, 6)),
            pltpu.SemaphoreType.DMA((2, SIDE, 6)),
            pltpu.SemaphoreType.DMA((2, 6)),
            pltpu.SemaphoreType.DMA((2, 6)),
            pltpu.SemaphoreType.DMA((2,)),
            pltpu.SemaphoreType.DMA((2,)),
        ],
        compiler_params=pltpu.CompilerParams(collective_id=0, has_side_effects=True, vmem_limit_bytes=60 * 1024 * 1024),
        name="scores",
    )(lengths, row_order, layer_inputs, out_grads, query_in, query_out)


def solution(mesh):
    placed = (P("seq", None, "feat"), P("seq", None, "feat"), P("seq"), P("seq"), P("feat", None), P("feat", None))
    return jax.shard_map(
        functools.partial(on_device, mesh.shape["seq"]),
        mesh=mesh, in_specs=placed, out_specs=P("seq", None), check_vma=False)
```

```python
import functools

import jax
import jax.numpy as jnp
from jax import lax
from jax.experimental import pallas as pl
from jax.experimental.pallas import tpu as pltpu
from jax.sharding import PartitionSpec as P

Q = 16
R = 32
SIDE = 4
LANES = 128
SUBLANES = 8
OFFS = (2, 1, 3, 0)
BF16 = jnp.bfloat16
F32 = jnp.float32


def kernel(n_seq, lengths_hbm, order_hbm, li, og, qi, qo, out,
           xb, gb, wi, wo, part, rec1, acc1, mid, rec2, acc2, early, tile, gz, mine, gp, lengths, row_order,
           load_sem, s1_send, s1_recv, s2_send, s2_recv, gz_sem, gp_sem, known):
    n_feat = SIDE * SIDE
    me_s = lax.axis_index("seq")
    me_f = lax.axis_index("feat")
    y = me_f // SIDE
    x = me_f % SIDE
    rows = xb.shape[2]
    seq_dev = li.shape[0]

    def neighbour(axis, step):
        if axis == 0:
            return y * SIDE + lax.rem(x + step, SIDE)
        return lax.rem(y + step, SIDE) * SIDE + x

    pos = (x, y)

    n_z = n_seq // 2
    z = me_s // 2
    core = lax.rem(me_s, 2)
    rounds = n_z // 2
    above_below = [{"seq": lax.rem(me_s + d, n_seq)} for d in (2, n_seq - 2)] if n_z > 1 else []
    nearby = [{"feat": neighbour(axis, d)} for axis in range(2) for d in (1, SIDE - 1)] + above_below
    if n_seq > 1:
        nearby.append({"seq": me_s + 1 - 2 * core})

    def signal(sem, target):
        pl.semaphore_signal(sem, inc=1, device_id=target, device_id_type=pl.DeviceIdType.MESH)

    barrier = pltpu.get_barrier_semaphore()
    for target in nearby:
        signal(barrier, target)

    def tell(r):
        if r < rounds:
            for target in above_below:
                signal(known.at[r], target)

    def heard(r):
        if r < rounds:
            pl.semaphore_wait(known.at[r], 2)

    def seq_of(h, t):
        return h * SIDE + lax.rem(pos[1 - h] + OFFS[t], SIDE)

    load_lengths = pltpu.make_async_copy(lengths_hbm, lengths, load_sem.at[18])
    load_order = pltpu.make_async_copy(order_hbm, row_order, load_sem.at[19])

    def load_x(h, t):
        return pltpu.make_async_copy(li.at[seq_of(h, t)], xb.at[h, t], load_sem.at[2 + h * 8 + t * 2])

    def load_g(h, t):
        return pltpu.make_async_copy(og.at[seq_of(h, t)], gb.at[h, t], load_sem.at[3 + h * 8 + t * 2])

    load_wi = pltpu.make_async_copy(qi, wi, load_sem.at[0])
    load_wo = pltpu.make_async_copy(qo, wo, load_sem.at[1])
    load_wi.start()
    load_x(0, 0).start()
    load_x(1, 0).start()
    load_wo.start()
    load_g(0, 0).start()
    load_g(1, 0).start()
    for h in range(2):
        load_x(h, 1).start()
        load_g(h, 1).start()

    def send(src, dst, ssem, rsem, target):
        copy = pltpu.make_async_remote_copy(
            src_ref=src, dst_ref=dst, send_sem=ssem, recv_sem=rsem,
            device_id={"feat": target}, device_id_type=pl.DeviceIdType.MESH)
        return copy

    def ring_copy(axis, slot, src, rec, ssem, rsem):
        step = 1 if slot in (0, 2, 5) else SIDE - 1
        return send(src, rec.at[slot], ssem.at[slot], rsem.at[slot], neighbour(axis, step))

    def tile_in(h, t, step):
        return part.at[h, t, lax.rem(pos[h] + step, SIDE)]

    def tile_out(h, t, step):
        return part.at[h, t, SIDE + lax.rem(pos[h] + step, SIDE)]

    def copy1(h, t, slot):
        if slot >= 4:
            src = acc1.at[h, t, slot - 4]
        elif slot in (0, 3):
            src = tile_in(h, t, 1 if slot == 0 else 2)
        else:
            src = tile_out(h, t, 3 if slot == 1 else 2)
        return ring_copy(h, slot, src, rec1.at[h, t], s1_send.at[h, t], s1_recv.at[h, t])

    def copy2(h, slot):
        src = (mid.at[h, 1, 0], mid.at[h, 2, 1], mid.at[h, 0, 1], mid.at[h, 0, 0], acc2.at[h, 0], acc2.at[h, 1])[slot]
        return ring_copy(1 - h, slot, src, rec2.at[h], s2_send.at[h], s2_recv.at[h])

    def added(*refs):
        total = refs[0][...].astype(F32)
        for ref in refs[1:]:
            total = total + ref[...].astype(F32)
        return total

    def compute_in(h, t):
        load_x(h, t).wait()
        value = jnp.dot(xb[h, t], wi[...], preferred_element_type=F32).astype(BF16)
        for c in range(SIDE):
            part[h, t, c] = value[:, c * LANES:(c + 1) * LANES]

    def compute_out(h, t):
        load_g(h, t).wait()
        value = jnp.dot(gb[h, t], wo[...], preferred_element_type=F32).astype(BF16)
        for c in range(SIDE):
            part[h, t, SIDE + c] = value[:, c * LANES:(c + 1) * LANES]

    def accumulate1(h, t):
        copy1(h, t, 3).wait_recv()
        acc1[h, t, 0] = added(tile_in(h, t, 3), rec1.at[h, t, 3]).astype(BF16)
        copy1(h, t, 4).start()
        copy1(h, t, 2).wait_recv()
        acc1[h, t, 1] = added(tile_out(h, t, 1), rec1.at[h, t, 2]).astype(BF16)
        copy1(h, t, 5).start()

    def final1(h, t):
        copy1(h, t, 0).wait_recv()
        copy1(h, t, 4).wait_recv()
        mid[h, t, 0] = added(tile_in(h, t, 0), rec1.at[h, t, 0], rec1.at[h, t, 4]).astype(BF16)
        copy1(h, t, 1).wait_recv()
        copy1(h, t, 5).wait_recv()
        mid[h, t, 1] = added(tile_out(h, t, 0), rec1.at[h, t, 1], rec1.at[h, t, 5]).astype(BF16)

    def send_in(t):
        for h in range(2):
            copy1(h, t, 3).start()
            copy1(h, t, 0).start()

    def send_out(t):
        for h in range(2):
            copy1(h, t, 2).start()
            copy1(h, t, 1).start()

    def load_later(t):
        for h in range(2):
            load_x(h, t).start()
            load_g(h, t).start()

    load_wi.wait()
    for h in range(2):
        compute_in(h, 0)
    pl.semaphore_wait(barrier, len(nearby))
    send_in(0)
    tell(0)
    load_wo.wait()
    for h in range(2):
        compute_out(h, 0)
    send_out(0)
    load_later(2)
    load_lengths.start()
    load_order.start()
    for h in range(2):
        compute_in(h, 1)
    send_in(1)
    for h in range(2):
        compute_out(h, 1)
    send_out(1)
    load_later(3)
    heard(0)
    tell(1)
    for h in range(2):
        accumulate1(h, 0)
    for h in range(2):
        compute_in(h, 2)
    send_in(2)
    for h in range(2):
        compute_out(h, 2)
    send_out(2)
    heard(1)
    tell(2)
    for h in range(2):
        accumulate1(h, 1)
    for h in range(2):
        final1(h, 0)
        copy2(h, 3).start()
        copy2(h, 2).start()
    heard(2)
    tell(3)
    for h in range(2):
        compute_in(h, 3)
        compute_out(h, 3)
    for h in range(2):
        accumulate1(h, 2)
    send_in(3)
    send_out(3)
    for h in range(2):
        final1(h, 1)
        copy2(h, 0).start()
    for h in range(2):
        copy2(h, 2).wait_recv()
        acc2[h, 1] = added(mid.at[h, 1, 1], rec2.at[h, 2]).astype(BF16)
        copy2(h, 5).start()
    for h in range(2):
        final1(h, 2)
        copy2(h, 1).start()
        copy2(h, 3).wait_recv()
        acc2[h, 0] = added(mid.at[h, 2, 0], rec2.at[h, 3]).astype(BF16)
        copy2(h, 4).start()
    for h in range(2):
        accumulate1(h, 3)
    for h in range(2):
        for side, own in enumerate((tile_in(h, 3, 0), tile_out(h, 3, 0))):
            copy1(h, 3, side).wait_recv()
            copy2(h, side).wait_recv()
            early[h, side] = added(own, rec1.at[h, 3, side], rec2.at[h, side])
    for h in range(2):
        for side in range(2):
            copy2(h, 4 + side).wait_recv()
            early[h, side] = added(early.at[h, side], rec2.at[h, 4 + side])
    heard(3)
    load_lengths.wait()
    load_order.wait()

    row = lax.broadcasted_iota(jnp.int32, (rows, LANES), 0)
    slot_row = lax.broadcasted_iota(jnp.int32, (SUBLANES, LANES), 0)
    sums = jnp.zeros((SUBLANES, LANES), F32)
    for h in range(2):
        live = row < lengths[seq_of(h, 3)]
        copy1(h, 3, 4).wait_recv()
        copy1(h, 3, 5).wait_recv()
        products = added(early.at[h, 0], rec1.at[h, 3, 4]) * added(early.at[h, 1], rec1.at[h, 3, 5])
        column_sums = jnp.sum(jnp.where(live, products, 0.0), axis=0, keepdims=True)
        sums = jnp.where(slot_row == h, column_sums, sums)
    high = sums.astype(BF16).astype(F32)
    middle = (sums - high).astype(BF16).astype(F32)
    low = sums - high - middle
    pieces = jnp.concatenate([high, middle, low], axis=0).astype(BF16)
    lane_from = lax.broadcasted_iota(jnp.int32, (LANES, LANES), 0)
    lane_to = lax.broadcasted_iota(jnp.int32, (LANES, LANES), 1)
    per_chunk = LANES // R
    group = (lane_from // R == lax.rem(lane_to, per_chunk)).astype(F32).astype(BF16)
    grouped = jnp.dot(pieces, group, preferred_element_type=F32)
    grouped = grouped[:SUBLANES] + grouped[SUBLANES:2 * SUBLANES] + grouped[2 * SUBLANES:]
    lane = lax.broadcasted_iota(jnp.int32, (SUBLANES, LANES), 1)
    chunk = lax.rem(lane, Q) // per_chunk
    scored = jnp.where(chunk == jnp.where(slot_row == 0, x, y), grouped, 0.0)[:2]
    tile[...] = scored
    gz[me_s] = scored

    def spread_z(dz, flip):
        target = lax.rem(z + dz, n_z) * 2 + (1 - core if flip else core)
        return pltpu.make_async_remote_copy(
            src_ref=tile, dst_ref=gz.at[me_s], send_sem=gz_sem.at[0], recv_sem=gz_sem.at[1],
            device_id={"seq": target}, device_id_type=pl.DeviceIdType.MESH)

    def spread_plane(dy, dx):
        target = lax.rem(y + dy, SIDE) * SIDE + lax.rem(x + dx, SIDE)
        return pltpu.make_async_remote_copy(
            src_ref=mine, dst_ref=gp.at[me_f], send_sem=gp_sem.at[0], recv_sem=gp_sem.at[1],
            device_id={"feat": target}, device_id_type=pl.DeviceIdType.MESH)

    def all_of(ref, sem, n, axis):
        return pltpu.make_async_remote_copy(
            src_ref=ref.at[pl.ds(0, n)], dst_ref=ref.at[pl.ds(0, n)], send_sem=sem.at[0], recv_sem=sem.at[1],
            device_id={axis: lax.axis_index(axis)}, device_id_type=pl.DeviceIdType.MESH)

    def hops(d, size):
        return min(d, size - d)

    far_first = sorted(((hops(dz, n_z), flip, dz) for dz in range(n_z) for flip in range(2)), reverse=True)
    for _, flip, dz in far_first:
        if dz or flip:
            if n_seq > 1:
                spread_z(dz, flip).start()
    for h in range(2):
        for t in range(SIDE):
            for slot in range(6):
                copy1(h, t, slot).wait_send()
        for slot in range(6):
            copy2(h, slot).wait_send()
    one_lane = lax.broadcasted_iota(jnp.int32, (1, LANES), 1) // Q
    picks = []
    for i in range(seq_dev):
        wanted = row_order[i]
        within = lax.rem(wanted, seq_dev)
        half = within // SIDE
        ours = lax.rem(within, SIDE) == jnp.where(half == 0, y, x)
        picks.append((wanted // seq_dev, half, jnp.where(ours, i, -1)))
    if n_seq > 1:
        all_of(gz, gz_sem, n_seq - 1, "seq").wait_recv()
    packed = jnp.zeros((1, LANES), F32)
    for who, half, place in picks:
        packed = jnp.where(one_lane == place, gz[who, pl.ds(half, 1), :], packed)
    mine[...] = packed
    gp[me_f] = packed
    far_first = sorted(((hops(dy, SIDE) + hops(dx, SIDE), dy, dx) for dy in range(SIDE) for dx in range(SIDE)), reverse=True)
    for _, dy, dx in far_first[:-1]:
        spread_plane(dy, dx).start()
    if n_seq > 1:
        all_of(gz, gz_sem, n_seq - 1, "seq").wait_send()
    all_of(gp, gp_sem, n_feat - 1, "feat").wait_recv()
    summed = gp[0]
    for f in range(1, n_feat):
        summed = summed + gp[f]
    spread = jnp.broadcast_to(summed, (seq_dev, LANES))
    lined = spread
    for i in range(1, seq_dev):
        lined = jnp.where(slot_row == i, pltpu.roll(spread, LANES - i * Q, 1), lined)
    out[...] = lined[:, :Q]
    all_of(gp, gp_sem, n_feat - 1, "feat").wait_send()


def on_device(n_seq, layer_inputs, out_grads, lengths, row_order, query_in, query_out):
    seq_dev, rows, width_in = layer_inputs.shape
    width_out = out_grads.shape[2]
    columns = query_in.shape[1]
    n_feat = SIDE * SIDE
    hbm = pl.BlockSpec(memory_space=pl.ANY)
    tile_of = (rows, LANES)
    return pl.pallas_call(
        functools.partial(kernel, n_seq),
        out_shape=pltpu.VMEM((seq_dev, Q), F32),
        in_specs=[hbm] * 6,
        out_specs=pl.BlockSpec(memory_space=pltpu.VMEM),
        scratch_shapes=[
            pltpu.VMEM((2, SIDE, rows, width_in), BF16),
            pltpu.VMEM((2, SIDE, rows, width_out), BF16),
            pltpu.VMEM((width_in, columns), BF16),
            pltpu.VMEM((width_out, columns), BF16),
            pltpu.VMEM((2, SIDE, 2 * SIDE, *tile_of), BF16),
            pltpu.VMEM((2, SIDE, 6, *tile_of), BF16),
            pltpu.VMEM((2, SIDE, 2, *tile_of), BF16),
            pltpu.VMEM((2, SIDE, 2, *tile_of), BF16),
            pltpu.VMEM((2, 6, *tile_of), BF16),
            pltpu.VMEM((2, 2, *tile_of), BF16),
            pltpu.VMEM((2, 2, *tile_of), F32),
            pltpu.VMEM((2, LANES), F32),
            pltpu.VMEM((n_seq, 2, LANES), F32),
            pltpu.VMEM((1, LANES), F32),
            pltpu.VMEM((n_feat, 1, LANES), F32),
            pltpu.SMEM((seq_dev,), jnp.int32),
            pltpu.SMEM((seq_dev,), jnp.int32),
            pltpu.SemaphoreType.DMA((20,)),
            pltpu.SemaphoreType.DMA((2, SIDE, 6)),
            pltpu.SemaphoreType.DMA((2, SIDE, 6)),
            pltpu.SemaphoreType.DMA((2, 6)),
            pltpu.SemaphoreType.DMA((2, 6)),
            pltpu.SemaphoreType.DMA((2,)),
            pltpu.SemaphoreType.DMA((2,)),
            pltpu.SemaphoreType.REGULAR((4,)),
        ],
        compiler_params=pltpu.CompilerParams(collective_id=0, has_side_effects=True, vmem_limit_bytes=60 * 1024 * 1024),
        name="scores",
    )(lengths, row_order, layer_inputs, out_grads, query_in, query_out)


def solution(mesh):
    placed = (P("seq", None, "feat"), P("seq", None, "feat"), P("seq"), P("seq"), P("feat", None), P("feat", None))
    return jax.shard_map(
        functools.partial(on_device, mesh.shape["seq"]),
        mesh=mesh, in_specs=placed, out_specs=P("seq", None), check_vma=False)
```

```python
import functools

import jax
import jax.numpy as jnp
from jax import lax
from jax.experimental import pallas as pl
from jax.experimental.pallas import tpu as pltpu
from jax.sharding import PartitionSpec as P

Q = 16
R = 32
SIDE = 4
LANES = 128
SUBLANES = 8
OFFS = (2, 1, 3, 0)
BF16 = jnp.bfloat16
F32 = jnp.float32


def kernel(n_seq, lengths_hbm, order_hbm, li, og, qi, qo, out,
           xb, gb, wi, wo, part, rec1, acc1, mid, rec2, acc2, early, tile, gz, mine, gp, lengths, row_order,
           load_sem, sent_sem, s1_recv, s2_recv, gz_sem, gp_sem, known):
    n_feat = SIDE * SIDE
    me_s = lax.axis_index("seq")
    me_f = lax.axis_index("feat")
    y = me_f // SIDE
    x = me_f % SIDE
    rows = xb.shape[2]
    last = SIDE - 1
    seq_dev = li.shape[0]

    def neighbour(axis, step):
        if axis == 0:
            return y * SIDE + lax.rem(x + step, SIDE)
        return lax.rem(y + step, SIDE) * SIDE + x

    pos = (x, y)

    n_z = n_seq // 2
    z = me_s // 2
    core = lax.rem(me_s, 2)
    rounds = n_z // 2
    above_below = [{"seq": lax.rem(me_s + d, n_seq)} for d in (2, n_seq - 2)] if n_z > 1 else []
    nearby = [{"feat": neighbour(axis, d)} for axis in range(2) for d in (1, SIDE - 1)] + above_below
    if n_seq > 1:
        nearby.append({"seq": me_s + 1 - 2 * core})

    def signal(sem, target):
        pl.semaphore_signal(sem, inc=1, device_id=target, device_id_type=pl.DeviceIdType.MESH)

    barrier = pltpu.get_barrier_semaphore()
    for target in nearby:
        signal(barrier, target)

    def tell(r):
        if r < rounds:
            for target in above_below:
                signal(known.at[r % 2], target)

    def heard(r):
        if r < rounds:
            pl.semaphore_wait(known.at[r % 2], 2)

    def seq_of(h, t):
        return h * SIDE + lax.rem(pos[1 - h] + OFFS[t], SIDE)

    load_lengths = pltpu.make_async_copy(lengths_hbm, lengths, load_sem.at[2 + 2 * SIDE])
    load_order = pltpu.make_async_copy(order_hbm, row_order, load_sem.at[3 + 2 * SIDE])

    def load_x(h, t):
        return pltpu.make_async_copy(li.at[seq_of(h, t)], xb.at[t, h], load_sem.at[2 + t])

    def load_g(h, t):
        return pltpu.make_async_copy(og.at[seq_of(h, t)], gb.at[t, h], load_sem.at[2 + SIDE + t])

    load_wi = pltpu.make_async_copy(qi, wi, load_sem.at[0])
    load_wo = pltpu.make_async_copy(qo, wo, load_sem.at[1])
    load_wi.start()
    load_x(0, 0).start()
    load_x(1, 0).start()
    load_wo.start()
    load_g(0, 0).start()
    load_g(1, 0).start()

    def send(src, dst, ssem, rsem, target):
        copy = pltpu.make_async_remote_copy(
            src_ref=src, dst_ref=dst, send_sem=ssem, recv_sem=rsem,
            device_id={"feat": target}, device_id_type=pl.DeviceIdType.MESH)
        return copy

    def ring_copy(axis, slot, src, rec, ssem, rsem):
        step = 1 if slot in (0, 2, 5) else SIDE - 1
        return send(src, rec.at[slot], ssem, rsem, neighbour(axis, step))

    def tile_in(h, t, step):
        return part.at[h, t, lax.rem(pos[h] + step, SIDE)]

    def tile_out(h, t, step):
        return part.at[h, t, SIDE + lax.rem(pos[h] + step, SIDE)]

    def sem1(h, t, slot):
        kind = (2, 2, 0, 1, 2, 2)[slot] + (1 if t == last and slot >= 4 else 0)
        return s1_recv.at[h * (3 * SIDE + 1) + 3 * t + kind]

    def sem2(h, slot):
        return s2_recv.at[h * 3 + (2, 2, 0, 1, 2, 2)[slot]]

    def copy1(h, t, slot):
        if slot >= 4:
            src = acc1.at[h, t, slot - 4]
        elif slot in (0, 3):
            src = tile_in(h, t, 1 if slot == 0 else 2)
        else:
            src = tile_out(h, t, 3 if slot == 1 else 2)
        return ring_copy(h, slot, src, rec1.at[h, t], sent_sem.at[0], sem1(h, t, slot))

    def copy2(h, slot):
        src = (mid.at[h, 1, 0], mid.at[h, 2, 1], mid.at[h, 0, 1], mid.at[h, 0, 0], acc2.at[h, 0], acc2.at[h, 1])[slot]
        return ring_copy(1 - h, slot, src, rec2.at[h], sent_sem.at[1], sem2(h, slot))

    def arrived(ref, sem):
        pltpu.make_async_remote_copy(
            src_ref=ref, dst_ref=ref, send_sem=sem, recv_sem=sem,
            device_id={"feat": me_f}, device_id_type=pl.DeviceIdType.MESH).wait_recv()

    def arrived1(h, t):
        arrived(rec1.at[h, t, pl.ds(0, 4)], sem1(h, t, 0))

    def added(*refs):
        total = refs[0][...].astype(F32)
        for ref in refs[1:]:
            total = total + ref[...].astype(F32)
        return total

    def compute_in(h, t):
        if h == 0:
            pltpu.make_async_copy(xb.at[t], xb.at[t], load_sem.at[2 + t]).wait()
        value = jnp.dot(xb[t, h], wi[...], preferred_element_type=F32).astype(BF16)
        for c in range(SIDE):
            part[h, t, c] = value[:, c * LANES:(c + 1) * LANES]

    def compute_out(h, t):
        if h == 0:
            pltpu.make_async_copy(gb.at[t], gb.at[t], load_sem.at[2 + SIDE + t]).wait()
        value = jnp.dot(gb[t, h], wo[...], preferred_element_type=F32).astype(BF16)
        for c in range(SIDE):
            part[h, t, SIDE + c] = value[:, c * LANES:(c + 1) * LANES]

    def accumulate1(h, t):
        copy1(h, t, 3).wait_recv()
        acc1[h, t, 0] = added(tile_in(h, t, 3), rec1.at[h, t, 3]).astype(BF16)
        copy1(h, t, 4).start()
        copy1(h, t, 2).wait_recv()
        acc1[h, t, 1] = added(tile_out(h, t, 1), rec1.at[h, t, 2]).astype(BF16)
        copy1(h, t, 5).start()

    def final1(h, t):
        arrived1(h, t)
        mid[h, t, 0] = added(tile_in(h, t, 0), rec1.at[h, t, 0], rec1.at[h, t, 4]).astype(BF16)
        mid[h, t, 1] = added(tile_out(h, t, 0), rec1.at[h, t, 1], rec1.at[h, t, 5]).astype(BF16)

    def send_in(h, t):
        copy1(h, t, 3).start()
        copy1(h, t, 0).start()

    def send_out(h, t):
        copy1(h, t, 2).start()
        copy1(h, t, 1).start()

    def load_later(t):
        for h in range(2):
            load_x(h, t).start()
            load_g(h, t).start()

    load_wi.wait()
    compute_in(0, 0)
    pl.semaphore_wait(barrier, len(nearby))
    send_in(0, 0)
    compute_in(1, 0)
    send_in(1, 0)
    load_later(1)
    tell(0)
    load_wo.wait()
    for h in range(2):
        compute_out(h, 0)
        send_out(h, 0)
    load_later(2)
    load_lengths.start()
    load_order.start()
    for h in range(2):
        compute_in(h, 1)
        send_in(h, 1)
    for h in range(2):
        compute_out(h, 1)
        send_out(h, 1)
    load_later(3)
    heard(0)
    tell(1)
    for h in range(2):
        accumulate1(h, 0)
    for h in range(2):
        compute_in(h, 2)
        send_in(h, 2)
    for h in range(2):
        compute_out(h, 2)
        send_out(h, 2)
    heard(1)
    tell(2)
    for h in range(2):
        accumulate1(h, 1)
    for h in range(2):
        final1(h, 0)
        copy2(h, 3).start()
        copy2(h, 2).start()
    heard(2)
    tell(3)
    for h in range(2):
        compute_in(h, 3)
        compute_out(h, 3)
    for h in range(2):
        accumulate1(h, 2)
    for h in range(2):
        send_in(h, 3)
        send_out(h, 3)
    for h in range(2):
        final1(h, 1)
        copy2(h, 0).start()
    for h in range(2):
        copy2(h, 2).wait_recv()
        acc2[h, 1] = added(mid.at[h, 1, 1], rec2.at[h, 2]).astype(BF16)
        copy2(h, 5).start()
    for h in range(2):
        final1(h, 2)
        copy2(h, 1).start()
        copy2(h, 3).wait_recv()
        acc2[h, 0] = added(mid.at[h, 2, 0], rec2.at[h, 3]).astype(BF16)
        copy2(h, 4).start()
    for h in range(2):
        accumulate1(h, 3)
    for h in range(2):
        arrived(rec1.at[h, last, pl.ds(0, 2)], sem1(h, last, 0))
        arrived(rec2.at[h, pl.ds(0, 4)], sem2(h, 0))
        for side, own in enumerate((tile_in(h, last, 0), tile_out(h, last, 0))):
            early[h, side] = added(own, rec1.at[h, last, side], rec2.at[h, side], rec2.at[h, 4 + side])
    heard(3)
    load_lengths.wait()
    load_order.wait()

    row = lax.broadcasted_iota(jnp.int32, (rows, LANES), 0)
    slot_row = lax.broadcasted_iota(jnp.int32, (SUBLANES, LANES), 0)
    sums = jnp.zeros((SUBLANES, LANES), F32)
    for h in range(2):
        live = row < lengths[seq_of(h, 3)]
        arrived(rec1.at[h, last, pl.ds(4, 2)], sem1(h, last, 4))
        products = added(early.at[h, 0], rec1.at[h, 3, 4]) * added(early.at[h, 1], rec1.at[h, 3, 5])
        column_sums = jnp.sum(jnp.where(live, products, 0.0), axis=0, keepdims=True)
        sums = jnp.where(slot_row == h, column_sums, sums)
    high = sums.astype(BF16).astype(F32)
    middle = (sums - high).astype(BF16).astype(F32)
    low = sums - high - middle
    pieces = jnp.concatenate([high, middle, low], axis=0).astype(BF16)
    lane_from = lax.broadcasted_iota(jnp.int32, (LANES, LANES), 0)
    lane_to = lax.broadcasted_iota(jnp.int32, (LANES, LANES), 1)
    per_chunk = LANES // R
    group = (lane_from // R == lax.rem(lane_to, per_chunk)).astype(F32).astype(BF16)
    grouped = jnp.dot(pieces, group, preferred_element_type=F32)
    grouped = grouped[:SUBLANES] + grouped[SUBLANES:2 * SUBLANES] + grouped[2 * SUBLANES:]
    lane = lax.broadcasted_iota(jnp.int32, (SUBLANES, LANES), 1)
    chunk = lax.rem(lane, Q) // per_chunk
    scored = jnp.where(chunk == jnp.where(slot_row == 0, x, y), grouped, 0.0)[:2]
    tile[...] = scored
    gz[me_s] = scored

    def spread_z(dz, flip):
        target = lax.rem(z + dz, n_z) * 2 + (1 - core if flip else core)
        return pltpu.make_async_remote_copy(
            src_ref=tile, dst_ref=gz.at[me_s], send_sem=gz_sem.at[0], recv_sem=gz_sem.at[1],
            device_id={"seq": target}, device_id_type=pl.DeviceIdType.MESH)

    def spread_plane(dy, dx):
        target = lax.rem(y + dy, SIDE) * SIDE + lax.rem(x + dx, SIDE)
        return pltpu.make_async_remote_copy(
            src_ref=mine, dst_ref=gp.at[me_f], send_sem=gp_sem.at[0], recv_sem=gp_sem.at[1],
            device_id={"feat": target}, device_id_type=pl.DeviceIdType.MESH)

    def all_of(ref, sem, n, axis):
        return pltpu.make_async_remote_copy(
            src_ref=ref.at[pl.ds(0, n)], dst_ref=ref.at[pl.ds(0, n)], send_sem=sem.at[0], recv_sem=sem.at[1],
            device_id={axis: lax.axis_index(axis)}, device_id_type=pl.DeviceIdType.MESH)

    def hops(d, size):
        return min(d, size - d)

    far_first = sorted(((hops(dz, n_z), flip, dz) for dz in range(n_z) for flip in range(2)), reverse=True)
    for _, flip, dz in far_first:
        if dz or flip:
            if n_seq > 1:
                spread_z(dz, flip).start()
    for ref, sem in ((rec1, sent_sem.at[0]), (rec2, sent_sem.at[1])):
        pltpu.make_async_remote_copy(
            src_ref=ref, dst_ref=ref, send_sem=sem, recv_sem=sem,
            device_id={"feat": me_f}, device_id_type=pl.DeviceIdType.MESH).wait_send()
    one_lane = lax.broadcasted_iota(jnp.int32, (1, LANES), 1) // Q
    picks = []
    for i in range(seq_dev):
        wanted = row_order[i]
        within = lax.rem(wanted, seq_dev)
        half = within // SIDE
        ours = lax.rem(within, SIDE) == jnp.where(half == 0, y, x)
        picks.append((wanted // seq_dev, half, jnp.where(ours, i, -1)))
    if n_seq > 1:
        all_of(gz, gz_sem, n_seq - 1, "seq").wait_recv()
    packed = jnp.zeros((1, LANES), F32)
    for who, half, place in picks:
        packed = jnp.where(one_lane == place, gz[who, pl.ds(half, 1), :], packed)
    mine[...] = packed
    gp[me_f] = packed
    far_first = sorted(((hops(dy, SIDE) + hops(dx, SIDE), dy, dx) for dy in range(SIDE) for dx in range(SIDE)), reverse=True)
    for _, dy, dx in far_first[:-1]:
        spread_plane(dy, dx).start()
    if n_seq > 1:
        all_of(gz, gz_sem, n_seq - 1, "seq").wait_send()
    all_of(gp, gp_sem, n_feat - 1, "feat").wait_recv()
    summed = gp[0]
    for f in range(1, n_feat):
        summed = summed + gp[f]
    spread = jnp.broadcast_to(summed, (seq_dev, LANES))
    lined = spread
    for i in range(1, seq_dev):
        lined = jnp.where(slot_row == i, pltpu.roll(spread, LANES - i * Q, 1), lined)
    out[...] = lined[:, :Q]
    all_of(gp, gp_sem, n_feat - 1, "feat").wait_send()


def on_device(n_seq, layer_inputs, out_grads, lengths, row_order, query_in, query_out):
    seq_dev, rows, width_in = layer_inputs.shape
    width_out = out_grads.shape[2]
    columns = query_in.shape[1]
    n_feat = SIDE * SIDE
    hbm = pl.BlockSpec(memory_space=pl.ANY)
    tile_of = (rows, LANES)
    return pl.pallas_call(
        functools.partial(kernel, n_seq),
        out_shape=pltpu.VMEM((seq_dev, Q), F32),
        in_specs=[hbm] * 6,
        out_specs=pl.BlockSpec(memory_space=pltpu.VMEM),
        scratch_shapes=[
            pltpu.VMEM((SIDE, 2, rows, width_in), BF16),
            pltpu.VMEM((SIDE, 2, rows, width_out), BF16),
            pltpu.VMEM((width_in, columns), BF16),
            pltpu.VMEM((width_out, columns), BF16),
            pltpu.VMEM((2, SIDE, 2 * SIDE, *tile_of), BF16),
            pltpu.VMEM((2, SIDE, 6, *tile_of), BF16),
            pltpu.VMEM((2, SIDE, 2, *tile_of), BF16),
            pltpu.VMEM((2, SIDE, 2, *tile_of), BF16),
            pltpu.VMEM((2, 6, *tile_of), BF16),
            pltpu.VMEM((2, 2, *tile_of), BF16),
            pltpu.VMEM((2, 2, *tile_of), F32),
            pltpu.VMEM((2, LANES), F32),
            pltpu.VMEM((n_seq, 2, LANES), F32),
            pltpu.VMEM((1, LANES), F32),
            pltpu.VMEM((n_feat, 1, LANES), F32),
            pltpu.SMEM((seq_dev,), jnp.int32),
            pltpu.SMEM((seq_dev,), jnp.int32),
            pltpu.SemaphoreType.DMA((4 + 2 * SIDE,)),
            pltpu.SemaphoreType.DMA((2,)),
            pltpu.SemaphoreType.DMA((2 * (3 * SIDE + 1),)),
            pltpu.SemaphoreType.DMA((6,)),
            pltpu.SemaphoreType.DMA((2,)),
            pltpu.SemaphoreType.DMA((2,)),
            pltpu.SemaphoreType.REGULAR((2,)),
        ],
        compiler_params=pltpu.CompilerParams(collective_id=0, has_side_effects=True, vmem_limit_bytes=60 * 1024 * 1024),
        name="scores",
    )(lengths, row_order, layer_inputs, out_grads, query_in, query_out)


def solution(mesh):
    placed = (P("seq", None, "feat"), P("seq", None, "feat"), P("seq"), P("seq"), P("feat", None), P("feat", None))
    return jax.shard_map(
        functools.partial(on_device, mesh.shape["seq"]),
        mesh=mesh, in_specs=placed, out_specs=P("seq", None), check_vma=False)
```

```python
import functools

import jax
import jax.numpy as jnp
from jax import lax
from jax.experimental import pallas as pl
from jax.experimental.pallas import tpu as pltpu
from jax.sharding import PartitionSpec as P

Q = 16
R = 32
SIDE = 4
LANES = 128
SUBLANES = 8
OFFS = (2, 1, 3, 0)
BF16 = jnp.bfloat16
F32 = jnp.float32


def kernel(n_seq, lengths_hbm, order_hbm, li, og, qi, qo, out,
           xb, gb, wi, wo, part, rec1, acc1, mid, rec2, acc2, early, tile, gz, mine, gp, lengths, row_order,
           load_sem, sent_sem, s1_recv, s2_recv, gz_sem, gp_sem, known):
    n_feat = SIDE * SIDE
    me_s = lax.axis_index("seq")
    me_f = lax.axis_index("feat")
    y = me_f // SIDE
    x = me_f % SIDE
    rows = xb.shape[2]
    last = SIDE - 1
    seq_dev = li.shape[0]

    def neighbour(axis, step):
        if axis == 0:
            return y * SIDE + lax.rem(x + step, SIDE)
        return lax.rem(y + step, SIDE) * SIDE + x

    pos = (x, y)

    n_z = n_seq // 2
    z = me_s // 2
    core = lax.rem(me_s, 2)
    rounds = n_z // 2
    above_below = [{"seq": lax.rem(me_s + d, n_seq)} for d in (2, n_seq - 2)] if n_z > 1 else []
    nearby = [{"feat": neighbour(axis, d)} for axis in range(2) for d in (1, SIDE - 1)] + above_below
    if n_seq > 1:
        nearby.append({"seq": me_s + 1 - 2 * core})

    def signal(sem, target):
        pl.semaphore_signal(sem, inc=1, device_id=target, device_id_type=pl.DeviceIdType.MESH)

    barrier = pltpu.get_barrier_semaphore()
    for target in nearby:
        signal(barrier, target)

    def tell(r):
        if r < rounds:
            for target in above_below:
                signal(known.at[r % 2], target)

    def heard(r):
        if r < rounds:
            pl.semaphore_wait(known.at[r % 2], 2)

    def seq_of(h, t):
        return h * SIDE + lax.rem(pos[1 - h] + OFFS[t], SIDE)

    load_lengths = pltpu.make_async_copy(lengths_hbm, lengths, load_sem.at[2 + 2 * SIDE])
    load_order = pltpu.make_async_copy(order_hbm, row_order, load_sem.at[3 + 2 * SIDE])

    def load_x(h, t):
        return pltpu.make_async_copy(li.at[seq_of(h, t)], xb.at[t, h], load_sem.at[2 + t])

    def load_g(h, t):
        return pltpu.make_async_copy(og.at[seq_of(h, t)], gb.at[t, h], load_sem.at[2 + SIDE + t])

    load_wi = pltpu.make_async_copy(qi, wi, load_sem.at[0])
    load_wo = pltpu.make_async_copy(qo, wo, load_sem.at[1])
    load_wi.start()
    load_x(0, 0).start()
    load_x(1, 0).start()
    load_wo.start()
    load_g(0, 0).start()
    load_g(1, 0).start()

    def send(src, dst, ssem, rsem, target):
        copy = pltpu.make_async_remote_copy(
            src_ref=src, dst_ref=dst, send_sem=ssem, recv_sem=rsem,
            device_id={"feat": target}, device_id_type=pl.DeviceIdType.MESH)
        return copy

    def ring_copy(axis, slot, src, rec, ssem, rsem):
        step = 1 if slot in (0, 2, 5) else SIDE - 1
        return send(src, rec.at[slot], ssem, rsem, neighbour(axis, step))

    def tile_in(h, t, step):
        return part.at[h, t, lax.rem(pos[h] + step, SIDE)]

    def tile_out(h, t, step):
        return part.at[h, t, SIDE + lax.rem(pos[h] + step, SIDE)]

    def sem1(h, t, slot):
        kind = (2, 2, 0, 1, 2, 2)[slot] + (1 if t == last and slot >= 4 else 0)
        return s1_recv.at[h * (3 * SIDE + 1) + 3 * t + kind]

    def sem2(h, slot):
        return s2_recv.at[h * 3 + (2, 2, 0, 1, 2, 2)[slot]]

    def copy1(h, t, slot):
        if slot >= 4:
            src = acc1.at[h, t, slot - 4]
        elif slot in (0, 3):
            src = tile_in(h, t, 1 if slot == 0 else 2)
        else:
            src = tile_out(h, t, 3 if slot == 1 else 2)
        return ring_copy(h, slot, src, rec1.at[h, t], sent_sem.at[0], sem1(h, t, slot))

    def copy2(h, slot):
        src = (mid.at[h, 1, 0], mid.at[h, 2, 1], mid.at[h, 0, 1], mid.at[h, 0, 0], acc2.at[h, 0], acc2.at[h, 1])[slot]
        return ring_copy(1 - h, slot, src, rec2.at[h], sent_sem.at[1], sem2(h, slot))

    def arrived(ref, sem):
        pltpu.make_async_remote_copy(
            src_ref=ref, dst_ref=ref, send_sem=sem, recv_sem=sem,
            device_id={"feat": me_f}, device_id_type=pl.DeviceIdType.MESH).wait_recv()

    def arrived1(h, t):
        arrived(rec1.at[h, t, pl.ds(0, 4)], sem1(h, t, 0))

    def added(*refs):
        total = refs[0][...].astype(F32)
        for ref in refs[1:]:
            total = total + ref[...].astype(F32)
        return total

    def compute_in(h, t):
        if h == 0:
            pltpu.make_async_copy(xb.at[t], xb.at[t], load_sem.at[2 + t]).wait()
        value = jnp.dot(xb[t, h], wi[...], preferred_element_type=F32).astype(BF16)
        for c in range(SIDE):
            part[h, t, c] = value[:, c * LANES:(c + 1) * LANES]

    def compute_out(h, t):
        if h == 0:
            pltpu.make_async_copy(gb.at[t], gb.at[t], load_sem.at[2 + SIDE + t]).wait()
        value = jnp.dot(gb[t, h], wo[...], preferred_element_type=F32).astype(BF16)
        for c in range(SIDE):
            part[h, t, SIDE + c] = value[:, c * LANES:(c + 1) * LANES]

    def accumulate1(h, t):
        copy1(h, t, 3).wait_recv()
        acc1[h, t, 0] = added(tile_in(h, t, 3), rec1.at[h, t, 3]).astype(BF16)
        copy1(h, t, 4).start()
        copy1(h, t, 2).wait_recv()
        acc1[h, t, 1] = added(tile_out(h, t, 1), rec1.at[h, t, 2]).astype(BF16)
        copy1(h, t, 5).start()

    def final1(h, t):
        arrived1(h, t)
        mid[h, t, 0] = added(tile_in(h, t, 0), rec1.at[h, t, 0], rec1.at[h, t, 4]).astype(BF16)
        mid[h, t, 1] = added(tile_out(h, t, 0), rec1.at[h, t, 1], rec1.at[h, t, 5]).astype(BF16)

    def send_in(h, t):
        copy1(h, t, 3).start()
        copy1(h, t, 0).start()

    def send_out(h, t):
        copy1(h, t, 2).start()
        copy1(h, t, 1).start()

    def far_first(t):
        for h in range(2):
            compute_in(h, t)
            copy1(h, t, 3).start()
        for h in range(2):
            compute_out(h, t)
            for slot in (2, 0, 1):
                copy1(h, t, slot).start()

    def load_later(t):
        for h in range(2):
            load_x(h, t).start()
            load_g(h, t).start()

    load_wi.wait()
    compute_in(0, 0)
    pl.semaphore_wait(barrier, len(nearby))
    send_in(0, 0)
    compute_in(1, 0)
    send_in(1, 0)
    load_later(1)
    tell(0)
    load_wo.wait()
    for h in range(2):
        compute_out(h, 0)
        send_out(h, 0)
    load_later(2)
    load_lengths.start()
    load_order.start()
    far_first(1)
    load_later(3)
    heard(0)
    tell(1)
    for h in range(2):
        accumulate1(h, 0)
    far_first(2)
    heard(1)
    tell(2)
    for h in range(2):
        accumulate1(h, 1)
    for h in range(2):
        compute_in(h, 3)
        compute_out(h, 3)
    for h in range(2):
        final1(h, 0)
        copy2(h, 3).start()
        copy2(h, 2).start()
    heard(2)
    tell(3)
    for h in range(2):
        accumulate1(h, 2)
    for h in range(2):
        for slot in (3, 2, 0, 1):
            copy1(h, 3, slot).start()
    for h in range(2):
        final1(h, 1)
        copy2(h, 0).start()
    for h in range(2):
        final1(h, 2)
        copy2(h, 1).start()
        copy2(h, 3).wait_recv()
        acc2[h, 0] = added(mid.at[h, 2, 0], rec2.at[h, 3]).astype(BF16)
        copy2(h, 4).start()
    for h in range(2):
        copy2(h, 2).wait_recv()
        acc2[h, 1] = added(mid.at[h, 1, 1], rec2.at[h, 2]).astype(BF16)
        copy2(h, 5).start()
    for h in range(2):
        accumulate1(h, 3)
    for h in range(2):
        arrived(rec1.at[h, last, pl.ds(0, 2)], sem1(h, last, 0))
        arrived(rec2.at[h, pl.ds(0, 4)], sem2(h, 0))
        for side, own in enumerate((tile_in(h, last, 0), tile_out(h, last, 0))):
            early[h, side] = added(own, rec1.at[h, last, side], rec2.at[h, side], rec2.at[h, 4 + side])
    heard(3)
    load_lengths.wait()
    load_order.wait()

    row = lax.broadcasted_iota(jnp.int32, (rows, LANES), 0)
    slot_row = lax.broadcasted_iota(jnp.int32, (SUBLANES, LANES), 0)
    sums = jnp.zeros((SUBLANES, LANES), F32)
    for h in range(2):
        live = row < lengths[seq_of(h, 3)]
        arrived(rec1.at[h, last, pl.ds(4, 2)], sem1(h, last, 4))
        products = added(early.at[h, 0], rec1.at[h, 3, 4]) * added(early.at[h, 1], rec1.at[h, 3, 5])
        column_sums = jnp.sum(jnp.where(live, products, 0.0), axis=0, keepdims=True)
        sums = jnp.where(slot_row == h, column_sums, sums)
    high = sums.astype(BF16).astype(F32)
    middle = (sums - high).astype(BF16).astype(F32)
    low = sums - high - middle
    pieces = jnp.concatenate([high, middle, low], axis=0).astype(BF16)
    lane_from = lax.broadcasted_iota(jnp.int32, (LANES, LANES), 0)
    lane_to = lax.broadcasted_iota(jnp.int32, (LANES, LANES), 1)
    per_chunk = LANES // R
    group = (lane_from // R == lax.rem(lane_to, per_chunk)).astype(F32).astype(BF16)
    grouped = jnp.dot(pieces, group, preferred_element_type=F32)
    grouped = grouped[:SUBLANES] + grouped[SUBLANES:2 * SUBLANES] + grouped[2 * SUBLANES:]
    lane = lax.broadcasted_iota(jnp.int32, (SUBLANES, LANES), 1)
    chunk = lax.rem(lane, Q) // per_chunk
    scored = jnp.where(chunk == jnp.where(slot_row == 0, x, y), grouped, 0.0)[:2]
    tile[...] = scored
    gz[me_s] = scored

    def spread_z(dz, flip):
        target = lax.rem(z + dz, n_z) * 2 + (1 - core if flip else core)
        return pltpu.make_async_remote_copy(
            src_ref=tile, dst_ref=gz.at[me_s], send_sem=gz_sem.at[0], recv_sem=gz_sem.at[1],
            device_id={"seq": target}, device_id_type=pl.DeviceIdType.MESH)

    def spread_plane(dy, dx):
        target = lax.rem(y + dy, SIDE) * SIDE + lax.rem(x + dx, SIDE)
        return pltpu.make_async_remote_copy(
            src_ref=mine, dst_ref=gp.at[me_f], send_sem=gp_sem.at[0], recv_sem=gp_sem.at[1],
            device_id={"feat": target}, device_id_type=pl.DeviceIdType.MESH)

    def all_of(ref, sem, n, axis):
        return pltpu.make_async_remote_copy(
            src_ref=ref.at[pl.ds(0, n)], dst_ref=ref.at[pl.ds(0, n)], send_sem=sem.at[0], recv_sem=sem.at[1],
            device_id={axis: lax.axis_index(axis)}, device_id_type=pl.DeviceIdType.MESH)

    def hops(d, size):
        return min(d, size - d)

    order = sorted(((hops(dz, n_z), flip, dz) for dz in range(n_z) for flip in range(2)), reverse=True)
    for _, flip, dz in order:
        if dz or flip:
            if n_seq > 1:
                spread_z(dz, flip).start()
    for ref, sem in ((rec1, sent_sem.at[0]), (rec2, sent_sem.at[1])):
        pltpu.make_async_remote_copy(
            src_ref=ref, dst_ref=ref, send_sem=sem, recv_sem=sem,
            device_id={"feat": me_f}, device_id_type=pl.DeviceIdType.MESH).wait_send()
    one_lane = lax.broadcasted_iota(jnp.int32, (1, LANES), 1) // Q
    picks = []
    for i in range(seq_dev):
        wanted = row_order[i]
        within = lax.rem(wanted, seq_dev)
        half = within // SIDE
        ours = lax.rem(within, SIDE) == jnp.where(half == 0, y, x)
        picks.append((wanted // seq_dev, half, jnp.where(ours, i, -1)))
    if n_seq > 1:
        all_of(gz, gz_sem, n_seq - 1, "seq").wait_recv()
    packed = jnp.zeros((1, LANES), F32)
    for who, half, place in picks:
        packed = jnp.where(one_lane == place, gz[who, pl.ds(half, 1), :], packed)
    mine[...] = packed
    gp[me_f] = packed
    order = sorted(((hops(dy, SIDE) + hops(dx, SIDE), dy, dx) for dy in range(SIDE) for dx in range(SIDE)), reverse=True)
    for _, dy, dx in order[:-1]:
        spread_plane(dy, dx).start()
    if n_seq > 1:
        all_of(gz, gz_sem, n_seq - 1, "seq").wait_send()
    all_of(gp, gp_sem, n_feat - 1, "feat").wait_recv()
    summed = gp[0]
    for f in range(1, n_feat):
        summed = summed + gp[f]
    spread = jnp.broadcast_to(summed, (seq_dev, LANES))
    lined = spread
    for i in range(1, seq_dev):
        lined = jnp.where(slot_row == i, pltpu.roll(spread, LANES - i * Q, 1), lined)
    out[...] = lined[:, :Q]
    all_of(gp, gp_sem, n_feat - 1, "feat").wait_send()


def on_device(n_seq, layer_inputs, out_grads, lengths, row_order, query_in, query_out):
    seq_dev, rows, width_in = layer_inputs.shape
    width_out = out_grads.shape[2]
    columns = query_in.shape[1]
    n_feat = SIDE * SIDE
    hbm = pl.BlockSpec(memory_space=pl.ANY)
    tile_of = (rows, LANES)
    return pl.pallas_call(
        functools.partial(kernel, n_seq),
        out_shape=pltpu.VMEM((seq_dev, Q), F32),
        in_specs=[hbm] * 6,
        out_specs=pl.BlockSpec(memory_space=pltpu.VMEM),
        scratch_shapes=[
            pltpu.VMEM((SIDE, 2, rows, width_in), BF16),
            pltpu.VMEM((SIDE, 2, rows, width_out), BF16),
            pltpu.VMEM((width_in, columns), BF16),
            pltpu.VMEM((width_out, columns), BF16),
            pltpu.VMEM((2, SIDE, 2 * SIDE, *tile_of), BF16),
            pltpu.VMEM((2, SIDE, 6, *tile_of), BF16),
            pltpu.VMEM((2, SIDE, 2, *tile_of), BF16),
            pltpu.VMEM((2, SIDE, 2, *tile_of), BF16),
            pltpu.VMEM((2, 6, *tile_of), BF16),
            pltpu.VMEM((2, 2, *tile_of), BF16),
            pltpu.VMEM((2, 2, *tile_of), F32),
            pltpu.VMEM((2, LANES), F32),
            pltpu.VMEM((n_seq, 2, LANES), F32),
            pltpu.VMEM((1, LANES), F32),
            pltpu.VMEM((n_feat, 1, LANES), F32),
            pltpu.SMEM((seq_dev,), jnp.int32),
            pltpu.SMEM((seq_dev,), jnp.int32),
            pltpu.SemaphoreType.DMA((4 + 2 * SIDE,)),
            pltpu.SemaphoreType.DMA((2,)),
            pltpu.SemaphoreType.DMA((2 * (3 * SIDE + 1),)),
            pltpu.SemaphoreType.DMA((6,)),
            pltpu.SemaphoreType.DMA((2,)),
            pltpu.SemaphoreType.DMA((2,)),
            pltpu.SemaphoreType.REGULAR((2,)),
        ],
        compiler_params=pltpu.CompilerParams(collective_id=0, has_side_effects=True, vmem_limit_bytes=60 * 1024 * 1024),
        name="scores",
    )(lengths, row_order, layer_inputs, out_grads, query_in, query_out)


def solution(mesh):
    placed = (P("seq", None, "feat"), P("seq", None, "feat"), P("seq"), P("seq"), P("feat", None), P("feat", None))
    return jax.shard_map(
        functools.partial(on_device, mesh.shape["seq"]),
        mesh=mesh, in_specs=placed, out_specs=P("seq", None), check_vma=False)
```
